32 devices in a mesh: depth: 16 (over z, y, x), spec: 2 (over core).
Axes of the slice: x: 2, y: 2, z: 4, core: 2. Of those that a mesh axis runs over, the one named last changes fastest.
Arguments:
- emission: bfloat16 [512, 64, 2048], P('depth', 'spec'), may hold values from 0.099609375 to 2
- opacity: bfloat16 [512, 64, 2048], P('depth', 'spec'), may hold values from 0.29882812 to 3
- bin_extinction: float32 [64], P('spec'), may hold values from 0.1 to 30
- entry: int32 [2048], replicated, may hold values from 0 to 127
- exit_cell: int32 [2048], replicated, may hold values from 384 to 512
- response: float32 [3, 64], P(None, 'spec'), may hold values from 0.05 to 1
Outputs:
- nearer_slab_rgb: float32 [16, 3, 2048], P('depth')
- image: float32 [3, 2048], replicated
The draws below stay inside these ranges and needn't reach their ends.
All inputs are finite; a program needn't handle non-finite values.
Results may differ from the reference program's by a relative error of at most 0.0003.
Values sent between devices are 32-bit elements; how exact they have to be, the bound alone decides.
A program may use at most 64 MiB of HBM per device.

```python
import math
import jax
import jax.numpy as jnp
from jax import lax

BINS = 64
CZ = 32
RAYS = 2048
DEPTH_SLABS = 16
NZ = 512


def place_ends(result, key, low, top_value):
    longest = result.shape.index(max(result.shape))
    spots = []
    for shift in (0, 1):
        where = [jax.random.randint(jax.random.fold_in(key, axis), (), 0, length) for axis, length in enumerate(result.shape)]
        where[longest] = (where[longest] + shift) % result.shape[longest]
        spots.append(tuple(where))
    return result.at[spots[0]].set(low).at[spots[1]].set(top_value)


def block_levels(rng, shape, cuts, least, largest):
    def one(axis_at, blocks):
        steps = jax.random.uniform(jax.random.fold_in(jax.random.fold_in(rng, 6), axis_at), (blocks,), jnp.float32, least / len(cuts), largest / len(cuts))
        return jnp.repeat(jnp.exp(steps), shape[axis_at] // blocks).reshape((-1,) + (1,) * (len(shape) - axis_at - 1))

    loudness = one(*cuts[0])
    for cut in cuts[1:]:
        loudness = loudness * one(*cut)
    return loudness


def setup_inputs(seed: int = 0) -> dict:
    key_list = jax.random.split(jax.random.key(seed), 7)
    emission = jnp.clip(jnp.exp(math.log(2.0) - 2.9996462 * jax.random.uniform(key_list[0], (NZ, BINS, RAYS), jnp.float32) ** block_levels(key_list[0], (NZ, BINS, RAYS), ((0, 16), (1, 2)), -0.2, 0.2)), 0.099609375, 2.0).astype(jnp.bfloat16)
    opacity = jnp.clip(jnp.exp(math.log(3.0) - 2.306499 * jax.random.uniform(key_list[1], (NZ, BINS, RAYS), jnp.float32) ** block_levels(key_list[1], (NZ, BINS, RAYS), ((0, 16), (1, 2)), -0.2, 0.2)), 0.29882812, 3.0).astype(jnp.bfloat16)
    bin_extinction = jnp.clip(jnp.exp(math.log(30.0) - 5.7037825 * jax.random.uniform(key_list[2], (BINS,), jnp.float32) ** block_levels(key_list[2], (BINS,), ((0, 2),), -0.2, 0.2)), 0.1, 30.0)
    entry = place_ends(jax.random.randint(key_list[3], (RAYS,), 0, NZ // 4), jax.random.fold_in(key_list[3], 1), 0, (NZ // 4) - 1).astype(jnp.int32)
    exit_cell = place_ends(jax.random.randint(key_list[4], (RAYS,), 3 * NZ // 4, NZ + 1), jax.random.fold_in(key_list[4], 1), 3 * NZ // 4, NZ).astype(jnp.int32)
    response = jnp.clip(0.05 + 0.95 * jax.random.uniform(key_list[5], (3, BINS), jnp.float32) ** block_levels(key_list[5], (3, BINS), ((1, 2),), -0.2, 0.2), 0.05, 1.0)
    return dict(emission=emission, opacity=opacity, bin_extinction=bin_extinction, entry=entry, exit_cell=exit_cell, response=response)


def merge_slabs(earlier, later):
    return (earlier[0] + earlier[1] * later[0], earlier[1] * later[1])


def reference(emission, opacity, bin_extinction, entry, exit_cell, response):
    cell_step = 1.0 / NZ
    emitted = emission.reshape(DEPTH_SLABS, CZ, BINS, RAYS)
    absorbed = opacity.reshape(DEPTH_SLABS, CZ, BINS, RAYS)

    def section_pass(inputs):
        glow, dense, section = inputs
        depth = section * CZ + jnp.arange(CZ, dtype=jnp.int32)
        inside = (depth[:, None] >= entry[None, :]) & (depth[:, None] < exit_cell[None, :])
        live = jnp.where(inside, 1.0, 0.0).astype(jnp.float32)
        tau = bin_extinction[None, :, None] * dense.astype(jnp.float32) * live[:, None, :] * cell_step
        running = jnp.cumsum(tau, axis=0)
        before = running - tau
        light = jnp.sum(glow.astype(jnp.float32) * live[:, None, :] * cell_step * jnp.exp(-before), axis=0)
        trans = jnp.exp(-(before[-1] + tau[-1]))
        return light, trans

    slab_radiances, transes = lax.map(section_pass, (emitted, absorbed, jnp.arange(DEPTH_SLABS, dtype=jnp.int32)))

    def advance(carry, pair):
        return merge_slabs(carry, pair), carry

    start = (jnp.zeros((BINS, RAYS), jnp.float32), jnp.ones((BINS, RAYS), jnp.float32))
    unused, fronts = lax.scan(advance, start, (slab_radiances, transes))
    nearer_radiance, nearer_transparency = fronts
    nearer_slab_rgb = jnp.einsum("ol,vlm->vom", response, nearer_radiance, precision=lax.Precision.HIGHEST)
    slab_colour_rgb = jnp.einsum("ol,vlm->vom", response, nearer_transparency * slab_radiances, precision=lax.Precision.HIGHEST)
    image = jnp.sum(slab_colour_rgb, axis=0)
    return nearer_slab_rgb, image
```

```python
import functools
import math
import jax
import jax.numpy as jnp
from jax import lax
from jax.experimental import pallas as pl
from jax.experimental.pallas import tpu as pltpu
from jax.sharding import PartitionSpec as P

LANES = 128
MESH = pl.DeviceIdType.MESH


def column(row, eye):
    return jnp.sum(jnp.where(eye, row, 0.0), axis=1, keepdims=True)


def kernel(
    groups, members, specs,
    em_hbm, op_hbm, ext_ref, entry_ref, exit_ref, resp_ref,
    near_ref, image_ref,
    em_v, op_v, s_out, s_in, l_out, l_in, z_in, z_out, c_own, c_sib, t_out, t_in, f_out, f_in,
    em_sem, op_sem, s_send, s_recv, l_send, l_recv, z_send, z_recv,
    c_send, c_recv, t_send, t_recv, f_send, f_recv,
):
    cells, bins, rays = em_hbm.shape
    part = rays // members
    tiles = part // LANES
    sections = groups * members
    cell_step = 1.0 / (cells * sections)
    me = lax.axis_index("depth")
    spec = lax.axis_index("spec")
    zi = me // members
    mi = me % members

    def owner(t):
        return lax.rem(mi + 1 + t, members)

    def rays_of(q):
        return pl.ds(pl.multiple_of(q * part, LANES), part)

    reads = []
    for hbm, vmem, sem in ((op_hbm, op_v, op_sem), (em_hbm, em_v, em_sem)):
        row = []
        for t in range(members):
            copy = pltpu.make_async_copy(hbm.at[:, :, rays_of(owner(t))], vmem.at[t], sem.at[t])
            copy.start()
            row.append(copy)
        reads.append(row)

    def peer_in_group(t):
        return (zi * members + owner(t), spec)

    outer = [(dz, ds) for dz in range(1, groups) for ds in range(specs)]

    def peer_outer(dz, ds):
        return (lax.rem(zi + dz, groups) * members + mi, lax.rem(spec + ds, specs))

    barrier = pltpu.get_barrier_semaphore()
    for t in range(members - 1):
        pl.semaphore_signal(barrier, inc=1, device_id=peer_in_group(t), device_id_type=MESH)
    for dz, ds in outer:
        pl.semaphore_signal(barrier, inc=1, device_id=peer_outer(dz, ds), device_id_type=MESH)
    for ds in range(1, specs):
        pl.semaphore_signal(
            barrier, inc=1, device_id=(me, lax.rem(spec + ds, specs)), device_id_type=MESH
        )

    eye = lax.broadcasted_iota(jnp.int32, (bins, bins), 0) == lax.broadcasted_iota(
        jnp.int32, (bins, bins), 1
    )
    scale = column(ext_ref[...].reshape(1, bins), eye) * (-cell_step * math.log2(math.e))
    scale = jnp.broadcast_to(scale, (bins, LANES))
    first = me * cells

    def bounds(q, j):
        at = pl.ds(pl.multiple_of(q * part + j * LANES, LANES), LANES)
        low = jnp.broadcast_to(entry_ref[at].reshape(1, LANES) - first, (8, LANES))
        high = jnp.broadcast_to(exit_ref[at].reshape(1, LANES) - first, (8, LANES))
        return low, high

    def live_at(i, low, high):
        return jnp.where((low <= i) & (high > i), 1.0, 0.0)

    def masked(x, live):
        return (x.astype(jnp.float32).reshape(bins // 8, 8, LANES) * live[None]).reshape(bins, LANES)

    def at_tile(j):
        return pl.ds(pl.multiple_of(j * LANES, LANES), LANES)

    sends = []
    for t in range(members):
        reads[0][t].wait()
        q = owner(t)

        @pl.loop(0, tiles)
        def _(j):
            low, high = bounds(q, j)
            total = jnp.zeros((bins, LANES), jnp.float32)
            for i in range(cells):
                total = total + masked(op_v[t, i, :, at_tile(j)], live_at(i, low, high))
            s_out[t, :, at_tile(j)] = total * scale

        if t == 0:
            pl.semaphore_wait(barrier, members - 1 + groups * specs - 1)
        if t < members - 1:
            copy = pltpu.make_async_remote_copy(
                s_out.at[t], s_in.at[mi], s_send.at[t], s_recv.at[mi],
                device_id=peer_in_group(t), device_id_type=MESH,
            )
            copy.start()
            sends.append(copy)

    for t in range(members):
        reads[1][t].wait()
        q = owner(t)

        @pl.loop(0, tiles)
        def _(j):
            low, high = bounds(q, j)
            run = jnp.zeros((bins, LANES), jnp.float32)
            glow = jnp.zeros((bins, LANES), jnp.float32)
            for i in range(cells):
                live = live_at(i, low, high)
                glow = glow + masked(em_v[t, i, :, at_tile(j)], live) * jnp.exp2(run)
                run = run + masked(op_v[t, i, :, at_tile(j)], live) * scale
            l_out[t, :, at_tile(j)] = glow * cell_step

        if t < members - 1:
            copy = pltpu.make_async_remote_copy(
                l_out.at[t], l_in.at[mi], l_send.at[t], l_recv.at[mi],
                device_id=peer_in_group(t), device_id_type=MESH,
            )
            copy.start()
            sends.append(copy)

    s_in[mi] = s_out[members - 1]
    l_in[mi] = l_out[members - 1]
    for t in range(members - 1):
        k = owner(t)
        pltpu.make_async_remote_copy(
            s_out.at[t], s_in.at[k], s_send.at[t], s_recv.at[k],
            device_id=peer_in_group(t), device_id_type=MESH,
        ).wait_recv()

    up = (lax.rem(zi + 1, groups) * members + mi, spec)

    def chain_copy(j):
        return pltpu.make_async_remote_copy(
            z_out.at[j], z_in.at[j], z_send.at[j], z_recv.at[j],
            device_id=up, device_id_type=MESH,
        )

    for j in range(tiles):
        lanes = pl.ds(j * LANES, LANES)
        here = s_in[0, :, lanes]
        for k in range(1, members):
            here = here + s_in[k, :, lanes]

        @pl.when(zi == 0)
        def _():
            z_in[j] = jnp.zeros((bins, LANES), jnp.float32)

        @pl.when(zi > 0)
        def _():
            chain_copy(j).wait_recv()

        @pl.when(zi < groups - 1)
        def _():
            z_out[j] = z_in[j] + here
            chain_copy(j).start()

    for t in range(members - 1):
        k = owner(t)
        pltpu.make_async_remote_copy(
            l_out.at[t], l_in.at[k], l_send.at[t], l_recv.at[k],
            device_id=peer_in_group(t), device_id_type=MESH,
        ).wait_recv()

    colours = resp_ref.shape[0]
    weights = [
        jnp.broadcast_to(column(resp_ref[pl.ds(c, 1), :], eye), (bins, LANES)) for c in range(colours)
    ]

    for j in range(tiles):
        lanes = pl.ds(j * LANES, LANES)
        ahead = z_in[j]
        totals = [None] * colours
        for k in range(members):
            seen = jnp.exp2(ahead) * l_in[k, :, lanes]
            for c in range(colours):
                value = jnp.sum(seen * weights[c], axis=0, keepdims=True)
                c_own[k, pl.ds(c, 1), lanes] = value
                totals[c] = value if k == 0 else totals[c] + value
            if k < members - 1:
                ahead = ahead + s_in[k, :, lanes]
        for c in range(colours):
            t_out[pl.ds(c, 1), lanes] = totals[c]

    for n, (dz, ds) in enumerate(outer):
        copy = pltpu.make_async_remote_copy(
            t_out, t_in.at[zi, spec], t_send.at[n], t_recv.at[zi, spec],
            device_id=peer_outer(dz, ds), device_id_type=MESH,
        )
        copy.start()
        sends.append(copy)
    for ds in range(1, specs):
        copy = pltpu.make_async_remote_copy(
            c_own, c_sib.at[spec], c_send.at[ds], c_recv.at[spec],
            device_id=(me, lax.rem(spec + ds, specs)), device_id_type=MESH,
        )
        copy.start()
        sends.append(copy)

    sums = [c_own[k] for k in range(members)]
    for ds in range(1, specs):
        other = lax.rem(spec + ds, specs)
        pltpu.make_async_remote_copy(
            c_own, c_sib.at[other], c_send.at[ds], c_recv.at[other],
            device_id=(me, other), device_id_type=MESH,
        ).wait_recv()
        sums = [sums[k] + c_sib[other, k] for k in range(members)]

    front = jnp.zeros((colours, part), jnp.float32)
    whole = sums[0]
    for k in range(1, members):
        whole = whole + sums[k]
    for n, (dz, ds) in enumerate(outer):
        z = lax.rem(zi + dz, groups)
        other = lax.rem(spec + ds, specs)
        pltpu.make_async_remote_copy(
            t_out, t_in.at[z, other], t_send.at[n], t_recv.at[z, other],
            device_id=peer_outer(dz, ds), device_id_type=MESH,
        ).wait_recv()
        value = t_in[z, other]
        front = front + value * jnp.where(z < zi, 1.0, 0.0)
        whole = whole + value

    for k in range(members):
        f_out[k, 0] = front
        f_out[k, 1] = whole
        if k < members - 1:
            front = front + sums[k]
    for t in range(members - 1):
        k = owner(t)
        copy = pltpu.make_async_remote_copy(
            f_out.at[k], f_in.at[mi], f_send.at[t], f_recv.at[mi],
            device_id=peer_in_group(t), device_id_type=MESH,
        )
        copy.start()
        sends.append(copy)
    near_ref[0, :, rays_of(mi)] = f_out[mi, 0]
    image_ref[:, rays_of(mi)] = f_out[mi, 1]
    for t in range(members - 1):
        k = owner(t)
        pltpu.make_async_remote_copy(
            f_out.at[k], f_in.at[k], f_send.at[t], f_recv.at[k],
            device_id=peer_in_group(t), device_id_type=MESH,
        ).wait_recv()
        near_ref[0, :, rays_of(k)] = f_in[k, 0]
        image_ref[:, rays_of(k)] = f_in[k, 1]

    for copy in sends:
        copy.wait_send()

    @pl.when(zi < groups - 1)
    def _():
        for j in range(tiles):
            chain_copy(j).wait_send()


def body(groups, members, specs, emission, opacity, bin_extinction, entry, exit_cell, response):
    cells, bins, rays = emission.shape
    colours = response.shape[0]
    part = rays // members
    tiles = part // LANES
    f32 = jnp.float32
    vmem = pl.BlockSpec(memory_space=pltpu.VMEM)
    hbm = pl.BlockSpec(memory_space=pltpu.HBM)
    dma = pltpu.SemaphoreType.DMA
    return pl.pallas_call(
        functools.partial(kernel, groups, members, specs),
        out_shape=(
            jax.ShapeDtypeStruct((1, colours, rays), f32),
            jax.ShapeDtypeStruct((colours, rays), f32),
        ),
        in_specs=[hbm, hbm, vmem, vmem, vmem, vmem],
        out_specs=(vmem, vmem),
        scratch_shapes=[
            pltpu.VMEM((members, cells, bins, part), emission.dtype),
            pltpu.VMEM((members, cells, bins, part), opacity.dtype),
            pltpu.VMEM((members, bins, part), f32),
            pltpu.VMEM((members, bins, part), f32),
            pltpu.VMEM((members, bins, part), f32),
            pltpu.VMEM((members, bins, part), f32),
            pltpu.VMEM((tiles, bins, LANES), f32),
            pltpu.VMEM((tiles, bins, LANES), f32),
            pltpu.VMEM((members, colours, part), f32),
            pltpu.VMEM((specs, members, colours, part), f32),
            pltpu.VMEM((colours, part), f32),
            pltpu.VMEM((groups, specs, colours, part), f32),
            pltpu.VMEM((members, 2, colours, part), f32),
            pltpu.VMEM((members, 2, colours, part), f32),
            dma((members,)), dma((members,)),
            dma((members,)), dma((members,)),
            dma((members,)), dma((members,)),
            dma((tiles,)), dma((tiles,)),
            dma((specs,)), dma((specs,)),
            dma((groups * specs,)), dma((groups, specs)),
            dma((members,)), dma((members,)),
        ],
        compiler_params=pltpu.CompilerParams(
            collective_id=0, has_side_effects=True, vmem_limit_bytes=56 * 2**20
        ),
    )(emission, opacity, bin_extinction, entry, exit_cell, response)


def solution(mesh):
    sections = mesh.shape["depth"]
    groups = next(g for g in range(1, sections + 1) if sections % g == 0 and g * g >= sections)
    placed = (
        P("depth", "spec", None),
        P("depth", "spec", None),
        P("spec"),
        P(),
        P(),
        P(None, "spec"),
    )
    return jax.shard_map(
        functools.partial(body, groups, sections // groups, mesh.shape["spec"]),
        mesh=mesh, in_specs=placed, out_specs=(P("depth", None, None), P()), check_vma=False,
    )
```

```python
import functools
import math
import jax
import jax.numpy as jnp
from jax import lax
from jax.experimental import pallas as pl
from jax.experimental.pallas import tpu as pltpu
from jax.sharding import PartitionSpec as P

LANES = 128
MESH = pl.DeviceIdType.MESH


def column(row, eye):
    return jnp.sum(jnp.where(eye, row, 0.0), axis=1, keepdims=True)


def kernel(
    groups, members, specs,
    em_hbm, op_hbm, ext_ref, entry_ref, exit_ref, resp_ref,
    near_ref, image_ref,
    em_v, op_v, s_out, s_in, l_out, l_in, z_in, z_out, c_own, c_sib, t_out, t_in, f_out, f_in,
    r_out, r_in, i_out, i_in, front_v, whole_v,
    em_sem, op_sem, s_send, s_recv, l_send, l_recv, z_send, z_recv,
    c_send, c_recv, t_send, t_recv, f_send, f_recv, r_send, r_recv, i_send, i_recv,
):
    cells, bins, rays = em_hbm.shape
    part = rays // members
    tiles = part // LANES
    sections = groups * members
    cell_step = 1.0 / (cells * sections)
    me = lax.axis_index("depth")
    spec = lax.axis_index("spec")
    zi = me // members
    mi = me % members

    def owner(t):
        return lax.rem(mi + 1 + t, members)

    def rays_of(q):
        return pl.ds(pl.multiple_of(q * part, LANES), part)

    reads = []
    for hbm, vmem, sem in ((op_hbm, op_v, op_sem), (em_hbm, em_v, em_sem)):
        row = []
        for t in range(members):
            copy = pltpu.make_async_copy(hbm.at[:, :, rays_of(owner(t))], vmem.at[t], sem.at[t])
            copy.start()
            row.append(copy)
        reads.append(row)

    def peer_in_group(t):
        return (zi * members + owner(t), spec)

    outer = [(dz, ds) for dz in range(1, groups) for ds in range(specs)]

    def peer_outer(dz, ds):
        return (lax.rem(zi + dz, groups) * members + mi, lax.rem(spec + ds, specs))

    barrier = pltpu.get_barrier_semaphore()
    for t in range(members - 1):
        pl.semaphore_signal(barrier, inc=1, device_id=peer_in_group(t), device_id_type=MESH)
    for dz, ds in outer:
        pl.semaphore_signal(barrier, inc=1, device_id=peer_outer(dz, ds), device_id_type=MESH)
    for ds in range(1, specs):
        pl.semaphore_signal(
            barrier, inc=1, device_id=(me, lax.rem(spec + ds, specs)), device_id_type=MESH
        )

    eye = lax.broadcasted_iota(jnp.int32, (bins, bins), 0) == lax.broadcasted_iota(
        jnp.int32, (bins, bins), 1
    )
    scale = column(ext_ref[...].reshape(1, bins), eye) * (-cell_step * math.log2(math.e))
    scale = jnp.broadcast_to(scale, (bins, LANES))
    first = me * cells

    def bounds(q, j):
        at = pl.ds(pl.multiple_of(q * part + j * LANES, LANES), LANES)
        low = jnp.broadcast_to(entry_ref[at].reshape(1, LANES) - first, (8, LANES))
        high = jnp.broadcast_to(exit_ref[at].reshape(1, LANES) - first, (8, LANES))
        return low, high

    def live_at(i, low, high):
        return jnp.where((low <= i) & (high > i), 1.0, 0.0)

    def masked(x, live):
        return (x.astype(jnp.float32).reshape(bins // 8, 8, LANES) * live[None]).reshape(bins, LANES)

    def at_tile(j):
        return pl.ds(pl.multiple_of(j * LANES, LANES), LANES)

    sends = []
    for t in range(members):
        reads[0][t].wait()
        q = owner(t)

        @pl.loop(0, tiles)
        def _(j):
            low, high = bounds(q, j)
            total = jnp.zeros((bins, LANES), jnp.float32)
            for i in range(cells):
                total = total + masked(op_v[t, i, :, at_tile(j)], live_at(i, low, high))
            s_out[t, :, at_tile(j)] = total * scale

        if t == 0:
            pl.semaphore_wait(barrier, members - 1 + groups * specs - 1)
        if t < members - 1:
            copy = pltpu.make_async_remote_copy(
                s_out.at[t], s_in.at[mi], s_send.at[t], s_recv.at[mi],
                device_id=peer_in_group(t), device_id_type=MESH,
            )
            copy.start()
            sends.append(copy)

    for t in range(members):
        reads[1][t].wait()
        q = owner(t)

        @pl.loop(0, tiles)
        def _(j):
            low, high = bounds(q, j)
            run = jnp.zeros((bins, LANES), jnp.float32)
            glow = jnp.zeros((bins, LANES), jnp.float32)
            for i in range(cells):
                live = live_at(i, low, high)
                glow = glow + masked(em_v[t, i, :, at_tile(j)], live) * jnp.exp2(run)
                run = run + masked(op_v[t, i, :, at_tile(j)], live) * scale
            l_out[t, :, at_tile(j)] = glow * cell_step

        if t < members - 1:
            copy = pltpu.make_async_remote_copy(
                l_out.at[t], l_in.at[mi], l_send.at[t], l_recv.at[mi],
                device_id=peer_in_group(t), device_id_type=MESH,
            )
            copy.start()
            sends.append(copy)

    s_in[mi] = s_out[members - 1]
    l_in[mi] = l_out[members - 1]
    for t in range(members - 1):
        k = owner(t)
        pltpu.make_async_remote_copy(
            s_out.at[t], s_in.at[k], s_send.at[t], s_recv.at[k],
            device_id=peer_in_group(t), device_id_type=MESH,
        ).wait_recv()

    half = groups // 2

    def wait_light():
        for t in range(members - 1):
            k = owner(t)
            pltpu.make_async_remote_copy(
                l_out.at[t], l_in.at[k], l_send.at[t], l_recv.at[k],
                device_id=peer_in_group(t), device_id_type=MESH,
            ).wait_recv()

    def group_light(lanes):
        ahead = s_in[0, :, lanes]
        light = l_in[0, :, lanes]
        for k in range(1, members):
            light = light + jnp.exp2(ahead) * l_in[k, :, lanes]
            ahead = ahead + s_in[k, :, lanes]
        return light, ahead

    down = (lax.rem(zi + groups - 1, groups) * members + mi, spec)

    def down_copy(j):
        return pltpu.make_async_remote_copy(
            r_out.at[j], r_in.at[j], r_send.at[j], r_recv.at[j],
            device_id=down, device_id_type=MESH,
        )

    @pl.when(zi > half)
    def _():
        wait_light()
        for j in range(tiles):
            light, depth = group_light(pl.ds(j * LANES, LANES))
            r_out[j] = light

            @pl.when(zi < groups - 1)
            def _():
                down_copy(j).wait_recv()
                r_out[j] = light + jnp.exp2(depth) * r_in[j]

            down_copy(j).start()

    up = (lax.rem(zi + 1, groups) * members + mi, spec)

    def chain_copy(j):
        return pltpu.make_async_remote_copy(
            z_out.at[j], z_in.at[j], z_send.at[j], z_recv.at[j],
            device_id=up, device_id_type=MESH,
        )

    for j in range(tiles):
        lanes = pl.ds(j * LANES, LANES)
        here = s_in[0, :, lanes]
        for k in range(1, members):
            here = here + s_in[k, :, lanes]

        @pl.when(zi == 0)
        def _():
            z_in[j] = jnp.zeros((bins, LANES), jnp.float32)

        @pl.when(zi > 0)
        def _():
            chain_copy(j).wait_recv()

        @pl.when(zi < groups - 1)
        def _():
            z_out[j] = z_in[j] + here
            chain_copy(j).start()

    @pl.when(zi <= half)
    def _():
        wait_light()

    colours = resp_ref.shape[0]
    weights = [
        jnp.broadcast_to(column(resp_ref[pl.ds(c, 1), :], eye), (bins, LANES)) for c in range(colours)
    ]

    everyone = [(dz, ds) for dz in range(groups) for ds in range(specs) if dz + ds > 0]

    def image_copy(n, source):
        return pltpu.make_async_remote_copy(
            i_out, i_in.at[source], i_send.at[n], i_recv.at[source],
            device_id=peer_outer(*everyone[n]), device_id_type=MESH,
        )

    @pl.when(zi == half)
    def _():
        for j in range(tiles):
            lanes = pl.ds(j * LANES, LANES)
            light, depth = group_light(lanes)
            if half < groups - 1:
                down_copy(j).wait_recv()
                light = light + jnp.exp2(depth) * r_in[j]
            seen = jnp.exp2(z_in[j]) * light
            for c in range(colours):
                i_out[pl.ds(c, 1), lanes] = jnp.sum(seen * weights[c], axis=0, keepdims=True)
        for n in range(len(everyone)):
            image_copy(n, spec).start()
        i_in[spec] = i_out[...]

    for j in range(tiles):
        lanes = pl.ds(j * LANES, LANES)
        ahead = z_in[j]
        totals = [None] * colours
        for k in range(members):
            seen = jnp.exp2(ahead) * l_in[k, :, lanes]
            for c in range(colours):
                value = jnp.sum(seen * weights[c], axis=0, keepdims=True)
                c_own[k, pl.ds(c, 1), lanes] = value
                totals[c] = value if k == 0 else totals[c] + value
            if k < members - 1:
                ahead = ahead + s_in[k, :, lanes]
        for c in range(colours):
            t_out[pl.ds(c, 1), lanes] = totals[c]

    def total_copy(n, z, source):
        return pltpu.make_async_remote_copy(
            t_out, t_in.at[z, source], t_send.at[n], t_recv.at[z, source],
            device_id=peer_outer(*outer[n]), device_id_type=MESH,
        )

    def needed(origin, reader):
        return (origin < half) | (reader > origin)

    for n, (dz, ds) in enumerate(outer):
        @pl.when(needed(zi, lax.rem(zi + dz, groups)))
        def _():
            total_copy(n, zi, spec).start()

    for ds in range(1, specs):
        copy = pltpu.make_async_remote_copy(
            c_own, c_sib.at[spec], c_send.at[ds], c_recv.at[spec],
            device_id=(me, lax.rem(spec + ds, specs)), device_id_type=MESH,
        )
        copy.start()
        sends.append(copy)

    sums = [c_own[k] for k in range(members)]
    for ds in range(1, specs):
        other = lax.rem(spec + ds, specs)
        pltpu.make_async_remote_copy(
            c_own, c_sib.at[other], c_send.at[ds], c_recv.at[other],
            device_id=(me, other), device_id_type=MESH,
        ).wait_recv()
        sums = [sums[k] + c_sib[other, k] for k in range(members)]

    front_v[...] = jnp.zeros((colours, part), jnp.float32)
    whole = sums[0]
    for k in range(1, members):
        whole = whole + sums[k]
    whole_v[...] = whole * jnp.where(zi < half, 1.0, 0.0)
    for n, (dz, ds) in enumerate(outer):
        z = lax.rem(zi + dz, groups)
        other = lax.rem(spec + ds, specs)

        @pl.when(needed(z, zi))
        def _():
            total_copy(n, z, other).wait_recv()
            value = t_in[z, other]
            front_v[...] = front_v[...] + value * jnp.where(z < zi, 1.0, 0.0)
            whole_v[...] = whole_v[...] + value * jnp.where(z < half, 1.0, 0.0)

    front = front_v[...]
    whole = whole_v[...]
    for source in range(specs):
        @pl.when((zi != half) | (spec != source))
        def _():
            image_copy(0, source).wait_recv()

        whole = whole + i_in[source]

    for k in range(members):
        f_out[k, 0] = front
        f_out[k, 1] = whole
        if k < members - 1:
            front = front + sums[k]
    for t in range(members - 1):
        k = owner(t)
        copy = pltpu.make_async_remote_copy(
            f_out.at[k], f_in.at[mi], f_send.at[t], f_recv.at[mi],
            device_id=peer_in_group(t), device_id_type=MESH,
        )
        copy.start()
        sends.append(copy)
    near_ref[0, :, rays_of(mi)] = f_out[mi, 0]
    image_ref[:, rays_of(mi)] = f_out[mi, 1]
    for t in range(members - 1):
        k = owner(t)
        pltpu.make_async_remote_copy(
            f_out.at[k], f_in.at[k], f_send.at[t], f_recv.at[k],
            device_id=peer_in_group(t), device_id_type=MESH,
        ).wait_recv()
        near_ref[0, :, rays_of(k)] = f_in[k, 0]
        image_ref[:, rays_of(k)] = f_in[k, 1]

    for copy in sends:
        copy.wait_send()

    for n, (dz, ds) in enumerate(outer):
        @pl.when(needed(zi, lax.rem(zi + dz, groups)))
        def _():
            total_copy(n, zi, spec).wait_send()

    @pl.when(zi < groups - 1)
    def _():
        for j in range(tiles):
            chain_copy(j).wait_send()

    @pl.when(zi > half)
    def _():
        for j in range(tiles):
            down_copy(j).wait_send()

    @pl.when(zi == half)
    def _():
        for n in range(len(everyone)):
            image_copy(n, spec).wait_send()


def place(near_ref, image_ref, near_out, image_out):
    for c in range(near_out.shape[0]):
        near_out[c] = near_ref[:, c]
    image_out[...] = image_ref[...]


def body(groups, members, specs, emission, opacity, bin_extinction, entry, exit_cell, response):
    cells, bins, rays = emission.shape
    colours = response.shape[0]
    part = rays // members
    tiles = part // LANES
    f32 = jnp.float32
    vmem = pl.BlockSpec(memory_space=pltpu.VMEM)
    hbm = pl.BlockSpec(memory_space=pltpu.HBM)
    dma = pltpu.SemaphoreType.DMA
    near, image = pl.pallas_call(
        functools.partial(kernel, groups, members, specs),
        out_shape=(
            jax.ShapeDtypeStruct((1, colours, rays), f32),
            jax.ShapeDtypeStruct((colours, rays), f32),
        ),
        in_specs=[hbm, hbm, vmem, vmem, vmem, vmem],
        out_specs=(vmem, vmem),
        scratch_shapes=[
            pltpu.VMEM((members, cells, bins, part), emission.dtype),
            pltpu.VMEM((members, cells, bins, part), opacity.dtype),
            pltpu.VMEM((members, bins, part), f32),
            pltpu.VMEM((members, bins, part), f32),
            pltpu.VMEM((members, bins, part), f32),
            pltpu.VMEM((members, bins, part), f32),
            pltpu.VMEM((tiles, bins, LANES), f32),
            pltpu.VMEM((tiles, bins, LANES), f32),
            pltpu.VMEM((members, colours, part), f32),
            pltpu.VMEM((specs, members, colours, part), f32),
            pltpu.VMEM((colours, part), f32),
            pltpu.VMEM((groups, specs, colours, part), f32),
            pltpu.VMEM((members, 2, colours, part), f32),
            pltpu.VMEM((members, 2, colours, part), f32),
            pltpu.VMEM((tiles, bins, LANES), f32),
            pltpu.VMEM((tiles, bins, LANES), f32),
            pltpu.VMEM((colours, part), f32),
            pltpu.VMEM((specs, colours, part), f32),
            pltpu.VMEM((colours, part), f32),
            pltpu.VMEM((colours, part), f32),
            dma((members,)), dma((members,)),
            dma((members,)), dma((members,)),
            dma((members,)), dma((members,)),
            dma((tiles,)), dma((tiles,)),
            dma((specs,)), dma((specs,)),
            dma((groups * specs,)), dma((groups, specs)),
            dma((members,)), dma((members,)),
            dma((tiles,)), dma((tiles,)),
            dma((groups * specs,)), dma((specs,)),
        ],
        compiler_params=pltpu.CompilerParams(
            collective_id=0, has_side_effects=True, vmem_limit_bytes=56 * 2**20
        ),
    )(emission, opacity, bin_extinction, entry, exit_cell, response)
    near, image = pl.pallas_call(
        place,
        out_shape=(
            jax.ShapeDtypeStruct((colours, 1, rays), f32),
            jax.ShapeDtypeStruct((colours, rays), f32),
        ),
        in_specs=[vmem, vmem],
        out_specs=(vmem, vmem),
    )(near, image)
    return jnp.transpose(near, (1, 0, 2)), image


def solution(mesh):
    sections = mesh.shape["depth"]
    groups = next(g for g in range(1, sections + 1) if sections % g == 0 and g * g >= sections)
    placed = (
        P("depth", "spec", None),
        P("depth", "spec", None),
        P("spec"),
        P(),
        P(),
        P(None, "spec"),
    )
    return jax.shard_map(
        functools.partial(body, groups, sections // groups, mesh.shape["spec"]),
        mesh=mesh, in_specs=placed, out_specs=(P("depth", None, None), P()), check_vma=False,
    )
```
